32 devices in a mesh: dp: 4 (over y, x), vocab: 8 (over z, core).
Axes of the slice: x: 2, y: 2, z: 4, core: 2. Of those that a mesh axis runs over, the one named last changes fastest.
Arguments:
- hidden: bfloat16 [512, 2048], P('dp'), may hold values from -6 to 6
- mix_weight: bfloat16 [2048, 4], replicated, may hold values from -0.125 to 0.125
- proj_weight: bfloat16 [4, 2048, 2048], P(None, None, 'vocab'), may hold values from -0.125 to 0.125
- out_weight: bfloat16 [2048, 32768], P(None, 'vocab'), may hold values from -0.15625 to 0.15625
- saved_lse: float32 [512, 4], P('dp'), may hold values from 1 to 30
- targets: int32 [512], P('dp'), may hold values from 0 to 32767
- loss_scale: float32 [512], P('dp'), may hold values from 4 to 32
Outputs:
- grad_hidden: bfloat16 [512, 2048], P('dp', 'vocab')
- grad_mix: float32 [2048, 4], P('dp')
- grad_proj: bfloat16 [4, 2048, 2048], P(None, 'dp', 'vocab')
- grad_out: bfloat16 [2048, 32768], P('dp', 'vocab')
The draws below stay inside these ranges and needn't reach their ends.
All inputs are finite; a program needn't handle non-finite values.
Results may differ from the reference program's by a relative error of at most 0.023.
Values may be sent and summed in bfloat16 or wider, within the bound.
A program may use at most 128 MiB of HBM per device.

```python
import math
import jax
import jax.numpy as jnp
from jax import lax

D = 2048
K = 4
TOK_DEV = 128
TOKENS = 512
VOCAB = 32768
N_DP = 4


def draw_saved_lse(key, part):
    center = jnp.log(jnp.float32(VOCAB)) - 1.9
    spread = jax.random.uniform(key, (TOKENS, K), jnp.float32, -0.3, 0.3)
    return (center + spread).astype(jnp.float32)


def draw_hidden(key, part):
    random_part = jax.random.normal(jax.random.fold_in(key, 11), (TOKENS, D), jnp.float32)
    values = random_part
    return jnp.clip(values, -6.0, 6.0).astype(jnp.bfloat16)


def touch_ends(values, rng, low, high):
    place = [jax.random.randint(jax.random.fold_in(rng, axis), (), 0, length) for axis, length in enumerate(values.shape)]
    widest = values.shape.index(max(values.shape))
    neighbour = place[:widest] + [(place[widest] + 1) % values.shape[widest]] + place[widest + 1:]
    return values.at[tuple(place)].set(low).at[tuple(neighbour)].set(high)


def steps_of(stream_key, extent, split, low, top_value):
    def one(position, blocks):
        heights = jax.random.uniform(jax.random.fold_in(jax.random.fold_in(stream_key, 6), position), (blocks,), jnp.float32, low / len(split), top_value / len(split))
        return jnp.repeat(jnp.exp(heights), extent[position] // blocks).reshape((-1,) + (1,) * (len(extent) - position - 1))

    loudness = one(*split[0])
    for cut in split[1:]:
        loudness = loudness * one(*cut)
    return loudness


def normal_values(stream_key, dims, scale, limit, pieces=(), kind=jnp.bfloat16):
    loudness = steps_of(stream_key, dims, pieces, -0.22, 0.18) if pieces else 1.0
    array = jax.random.normal(stream_key, dims, jnp.float32) * scale * loudness
    return jnp.minimum(jnp.maximum(array, -limit), limit).astype(kind)


def setup_inputs(seed: int = 0) -> dict:
    key_list = jax.random.split(jax.random.key(seed), 8)
    hidden = draw_hidden(jax.random.fold_in(key_list[7], 71), 0)
    mix_weight = normal_values(key_list[1], (D, K), D ** -0.5, 0.125)
    proj_weight = normal_values(key_list[2], (K, D, D), D ** -0.5, 0.125, ((2, 8),))
    out_weight = normal_values(key_list[3], (D, VOCAB), (4 * D // 5) ** -0.5, 0.15625, ((1, 8),))
    saved_lse = draw_saved_lse(jax.random.fold_in(key_list[7], 71), 0)
    targets = touch_ends(jax.random.randint(key_list[5], (TOKENS,), 0, VOCAB), jax.random.fold_in(key_list[5], 1), 0, VOCAB - 1).astype(jnp.int32)
    loss_scale = jnp.clip(jnp.exp(math.log(32.0) - 2.0794415 * jax.random.uniform(key_list[6], (TOKENS,), jnp.float32) ** steps_of(key_list[6], (TOKENS,), ((0, 4),), -0.2, 0.2)), 4.0, 32.0)
    return dict(hidden=hidden, mix_weight=mix_weight, proj_weight=proj_weight, out_weight=out_weight, saved_lse=saved_lse, targets=targets, loss_scale=loss_scale)


def reference(hidden, mix_weight, proj_weight, out_weight, saved_lse, targets, loss_scale):
    proj_float = proj_weight.astype(jnp.float32)
    mix_float = mix_weight.astype(jnp.float32)
    vocab_total = out_weight.shape[1]
    hidden_groups = hidden.reshape(N_DP, TOK_DEV, D)
    lse_groups = saved_lse.reshape(N_DP, TOK_DEV, K)
    target_groups = targets.reshape(N_DP, TOK_DEV)
    scale_groups = loss_scale.reshape(N_DP, TOK_DEV)

    def group_step(carry, inputs):
        embed_acc, proj_acc, mix_acc = carry
        group_hidden, group_lse, group_targets, group_scale = inputs
        hidden_float = group_hidden.astype(jnp.float32)
        mix_logits = jnp.dot(group_hidden, mix_weight, preferred_element_type=jnp.float32)
        log_mix = mix_logits - jnp.log(jnp.sum(jnp.exp(mix_logits), axis=1, keepdims=True))
        mix_prob = jnp.exp(log_mix)
        pre_act = jnp.einsum("td,kde->tke", hidden_float, proj_float, precision=lax.Precision.HIGHEST)
        comp = jnp.tanh(pre_act).astype(jnp.bfloat16)
        comp_rows = comp.reshape(TOK_DEV * K, D)
        logits = jnp.dot(comp_rows, out_weight, preferred_element_type=jnp.float32)
        lse_flat = group_lse.reshape(TOK_DEV * K)
        probabilities = jnp.exp(logits - lse_flat[:, None])
        target_rows = jnp.broadcast_to(group_targets[:, None], (TOK_DEV, K)).reshape(TOK_DEV * K).astype(jnp.int32)
        target_logit = jnp.take_along_axis(logits, target_rows[:, None], axis=1)[:, 0].reshape(TOK_DEV, K)
        weights = jnp.exp(log_mix + target_logit - group_lse)
        responsibility = weights / jnp.sum(weights, axis=1, keepdims=True)
        coefficient = (group_scale[:, None] * responsibility).reshape(TOK_DEV * K)
        onehot = (jnp.arange(vocab_total, dtype=jnp.int32)[None, :] == target_rows[:, None]).astype(jnp.float32)
        grad_logits = (coefficient[:, None] * (probabilities - onehot)).astype(jnp.bfloat16)
        embed_term = jnp.dot(comp_rows.T, grad_logits, preferred_element_type=jnp.float32)
        embed_round = lax.optimization_barrier(embed_term.astype(jnp.bfloat16)).astype(jnp.float32)
        grad_comp = jnp.dot(grad_logits, out_weight.T, preferred_element_type=jnp.float32)
        comp_float = comp.astype(jnp.float32)
        grad_pre = (grad_comp.reshape(TOK_DEV, K, D) * (1.0 - comp_float * comp_float)).astype(jnp.bfloat16)
        pre_float = grad_pre.astype(jnp.float32)
        proj_term = jnp.einsum("td,tke->kde", hidden_float, pre_float, precision=lax.Precision.HIGHEST)
        grad_mix_logit = -group_scale[:, None] * (responsibility - mix_prob)
        mix_term = jnp.dot(hidden_float.T, grad_mix_logit, precision=lax.Precision.HIGHEST)
        hidden_grad = jnp.einsum("tke,kde->td", pre_float, proj_float, precision=lax.Precision.HIGHEST)
        hidden_grad = hidden_grad + jnp.dot(grad_mix_logit, mix_float.T, precision=lax.Precision.HIGHEST)
        new_carry = (embed_acc + embed_round, proj_acc + proj_term, mix_acc + mix_term)
        return new_carry, hidden_grad.astype(jnp.bfloat16)

    initial = (jnp.zeros((D, vocab_total), jnp.float32), jnp.zeros((K, D, D), jnp.float32), jnp.zeros((D, K), jnp.float32))
    totals, hidden_grads = lax.scan(group_step, initial, (hidden_groups, lse_groups, target_groups, scale_groups))
    embed_acc, proj_acc, mix_acc = totals
    grad_hidden = hidden_grads.reshape(N_DP * TOK_DEV, D)
    return grad_hidden, mix_acc, proj_acc.astype(jnp.bfloat16), embed_acc.astype(jnp.bfloat16)
```

```python
import jax
import jax.numpy as jnp
from jax import lax
from jax.sharding import PartitionSpec as P

F32 = jnp.float32
BF16 = jnp.bfloat16


def swap(x, axis, size, s):
    return lax.ppermute(x, axis, [(i, i ^ s) for i in range(size)])


def shards(dp, nv, hidden, mix_weight, proj_weight, out_weight, saved_lse, targets, loss_scale):
    tokens, width = hidden.shape
    comps, _, cols = proj_weight.shape
    vocab_local = out_weight.shape[1]
    vi = lax.axis_index("vocab")
    di = lax.axis_index("dp")
    rows = tokens * comps
    dblk = width // dp

    mix_logits = jnp.dot(hidden, mix_weight, preferred_element_type=F32).T
    log_mix = mix_logits - jnp.log(jnp.sum(jnp.exp(mix_logits), axis=0, keepdims=True))
    mix_prob = jnp.exp(log_mix)
    lse = saved_lse.T

    pre = jnp.einsum("td,kde->kte", hidden, proj_weight, preferred_element_type=F32)
    comp_local = jnp.tanh(pre).astype(BF16)
    comp_all = lax.all_gather(comp_local, "vocab", axis=2, tiled=True)
    comp_rows = comp_all.reshape(rows, width)

    local_t = jnp.broadcast_to(targets.astype(F32)[None], (comps, tokens))
    info = jnp.stack([lse, local_t])
    infos = [info] + [swap(info, "dp", dp, s) for s in range(1, dp)]

    def hid_block(s):
        return lax.dynamic_slice_in_dim(hidden, (di ^ s) * dblk, dblk, 1)

    hid_blocks = [hid_block(0)] + [swap(hid_block(s), "dp", dp, s) for s in range(1, dp)]

    core = vi % 2
    half = lax.dynamic_slice_in_dim(comp_rows, core * (rows // 2), rows // 2, 0)
    got = [swap(half, "dp", dp, s) for s in range(1, dp)]
    other = [swap(h, "vocab", nv, 1) for h in got]
    parts = []
    for h, o in zip(got, other):
        parts.append(jnp.where(core == 0, h, o))
        parts.append(jnp.where(core == 0, o, h))
    comp_others = jnp.concatenate(parts, axis=0)

    iota = lax.broadcasted_iota(jnp.int32, (1, vocab_local), 1)

    def soft(comp, lse_r, tgt_r):
        logits = jnp.dot(comp, out_weight, preferred_element_type=F32)
        hot = iota == (tgt_r.astype(jnp.int32) - vi * vocab_local)[:, None]
        p = (jnp.exp(logits - lse_r[:, None]) - hot.astype(F32)).astype(BF16)
        return p, logits, hot

    p_own, logits, hot = soft(comp_rows, lse.reshape(rows), local_t.reshape(rows))
    t_part = jnp.sum(jnp.where(hot, logits, 0.0), axis=1).reshape(comps, tokens)
    s = 1
    while s < nv:
        t_part = t_part + swap(t_part, "vocab", nv, s)
        s *= 2
    target_logit = t_part
    w = jnp.exp(log_mix + target_logit - lse)
    resp = w / jnp.sum(w, axis=0, keepdims=True)
    coef = loss_scale[None] * resp
    gml = -loss_scale[None] * (resp - mix_prob)
    scal = jnp.stack([coef, gml])
    scals = [scal] + [swap(scal, "dp", dp, s) for s in range(1, dp)]

    gc = lax.dot_general(p_own, out_weight, (((1,), (1,)), ((), ())), preferred_element_type=F32)
    gc = (gc * coef.reshape(rows)[:, None]).astype(BF16)
    gc = lax.psum_scatter(gc, "vocab", scatter_dimension=1, tiled=True)

    lse_o = jnp.concatenate([i[0].reshape(rows) for i in infos[1:]])
    tgt_o = jnp.concatenate([i[1].reshape(rows) for i in infos[1:]])
    p_others = soft(comp_others, lse_o, tgt_o)[0]

    cf = comp_local.astype(F32)
    grad_pre = (gc.astype(F32).reshape(comps, tokens, cols) * (1.0 - cf * cf)).astype(BF16)
    hidden_term = jnp.einsum("kte,kde->td", grad_pre, proj_weight, preferred_element_type=F32)
    hidden_part = lax.psum_scatter(
        hidden_term.astype(BF16), "vocab", scatter_dimension=1, tiled=True
    ).astype(F32)
    pres = [grad_pre] + [swap(grad_pre, "dp", dp, s) for s in range(1, dp)]
    pre_all = jnp.concatenate(pres, axis=1)
    hid_all = jnp.concatenate(hid_blocks, axis=0)
    grad_proj = jnp.einsum("td,kte->kde", hid_all, pre_all, preferred_element_type=F32).astype(BF16)

    def scaled(c, k):
        blk = lax.dynamic_slice_in_dim(c, di * dblk, dblk, 1).astype(F32)
        return (blk * k[:, None]).astype(BF16)

    def back(c, p):
        return lax.dot_general(c, p, (((0,), (0,)), ((), ())), preferred_element_type=F32)

    coef_o = jnp.concatenate([c[0].reshape(rows) for c in scals[1:]])
    grad_out = back(scaled(comp_others, coef_o), p_others)
    grad_out = (grad_out + back(scaled(comp_rows, coef.reshape(rows)), p_own)).astype(BF16)

    gml_all = jnp.concatenate([c[1] for c in scals], axis=1)
    grad_mix = lax.dot_general(
        hid_all.astype(F32), gml_all, (((0,), (1,)), ((), ())), precision=lax.Precision.HIGHEST
    )
    mix_rows = lax.dynamic_slice_in_dim(mix_weight, vi * cols, cols, 0).astype(F32)
    mix_term = lax.dot_general(
        gml, mix_rows, (((0,), (1,)), ((), ())), precision=lax.Precision.HIGHEST
    )
    grad_hidden = (hidden_part + mix_term).astype(BF16)
    return grad_hidden, grad_mix, grad_proj, grad_out


def solution(mesh):
    dp, nv = mesh.shape["dp"], mesh.shape["vocab"]

    def body(*args):
        return shards(dp, nv, *args)

    return jax.shard_map(
        body,
        mesh=mesh,
        in_specs=(
            P("dp", None),
            P(),
            P(None, None, "vocab"),
            P(None, "vocab"),
            P("dp", None),
            P("dp"),
            P("dp"),
        ),
        out_specs=(P("dp", "vocab"), P("dp", None), P(None, "dp", "vocab"), P("dp", "vocab")),
        check_vma=False,
    )
```

```python
import jax
import jax.numpy as jnp
from jax import lax
from jax.sharding import PartitionSpec as P

F32 = jnp.float32
BF16 = jnp.bfloat16


def swap(x, axis, size, s):
    return lax.ppermute(x, axis, [(i, i ^ s) for i in range(size)])


def shards(dp, nv, hidden, mix_weight, proj_weight, out_weight, saved_lse, targets, loss_scale):
    tokens, width = hidden.shape
    comps, _, cols = proj_weight.shape
    vocab_local = out_weight.shape[1]
    vi = lax.axis_index("vocab")
    di = lax.axis_index("dp")
    rows = tokens * comps
    dblk = width // dp

    mix_logits = jnp.dot(hidden, mix_weight, preferred_element_type=F32).T
    log_mix = mix_logits - jnp.log(jnp.sum(jnp.exp(mix_logits), axis=0, keepdims=True))
    mix_prob = jnp.exp(log_mix)
    lse = saved_lse.T

    pre = jnp.einsum("td,kde->kte", hidden, proj_weight, preferred_element_type=F32)
    comp_local = jnp.tanh(pre).astype(BF16)
    comp_all = lax.all_gather(comp_local, "vocab", axis=2, tiled=True)
    comp_rows = comp_all.reshape(rows, width)

    local_t = jnp.broadcast_to(targets.astype(F32)[None], (comps, tokens))
    info = jnp.stack([lse, local_t])
    infos = [info] + [swap(info, "dp", dp, s) for s in range(1, dp)]

    def hid_block(s):
        return lax.dynamic_slice_in_dim(hidden, (di ^ s) * dblk, dblk, 1)

    hid_blocks = [hid_block(0)] + [swap(hid_block(s), "dp", dp, s) for s in range(1, dp)]

    core = vi % 2
    half = lax.dynamic_slice_in_dim(comp_rows, core * (rows // 2), rows // 2, 0)
    got = [swap(half, "dp", dp, s) for s in range(1, dp)]

    iota = lax.broadcasted_iota(jnp.int32, (1, vocab_local), 1)

    def soft(comp, lse_r, tgt_r):
        logits = jnp.dot(comp, out_weight, preferred_element_type=F32)
        hot = iota == (tgt_r.astype(jnp.int32) - vi * vocab_local)[:, None]
        p = (jnp.exp(logits - lse_r[:, None]) - hot.astype(F32)).astype(BF16)
        return p, logits, hot

    p_own, logits, hot = soft(comp_rows, lse.reshape(rows), local_t.reshape(rows))
    t_part = jnp.sum(jnp.where(hot, logits, 0.0), axis=1).reshape(comps, tokens)
    s = 1
    while s < nv:
        t_part = t_part + swap(t_part, "vocab", nv, s)
        s *= 2
    w = jnp.exp(log_mix + t_part - lse)
    resp = w / jnp.sum(w, axis=0, keepdims=True)
    coef = loss_scale[None] * resp
    gml = -loss_scale[None] * (resp - mix_prob)
    scal = jnp.stack([coef, gml])
    scals = [scal] + [swap(scal, "dp", dp, s) for s in range(1, dp)]

    gc = lax.dot_general(
        p_own, out_weight, (((1,), (1,)), ((), ())), preferred_element_type=F32
    ).astype(BF16)
    gc = lax.psum_scatter(gc, "vocab", scatter_dimension=1, tiled=True)
    other = [swap(h, "vocab", nv, 1) for h in got]

    def rows_of(picks):
        parts = []
        for s in picks:
            parts.append(jnp.where(core == 0, got[s - 1], other[s - 1]))
            parts.append(jnp.where(core == 0, other[s - 1], got[s - 1]))
        return jnp.concatenate(parts, axis=0)

    def scaled(c, k):
        blk = lax.dynamic_slice_in_dim(c, di * dblk, dblk, 1).astype(F32)
        return (blk * k[:, None]).astype(BF16)

    def back(c, p):
        return lax.dot_general(c, p, (((0,), (0,)), ((), ())), preferred_element_type=F32)

    def contribution(picks, comp):
        lse_o = jnp.concatenate([infos[s][0].reshape(rows) for s in picks])
        tgt_o = jnp.concatenate([infos[s][1].reshape(rows) for s in picks])
        coef_o = jnp.concatenate([scals[s][0].reshape(rows) for s in picks])
        return back(scaled(comp, coef_o), soft(comp, lse_o, tgt_o)[0])

    first, second = list(range(1, (dp + 2) // 2)), list(range((dp + 2) // 2, dp))
    grad_out = contribution(first, rows_of(first))

    cf = comp_local.astype(F32)
    gc = gc.astype(F32).reshape(comps, tokens, cols) * coef[:, :, None]
    grad_pre = (gc * (1.0 - cf * cf)).astype(BF16)
    hidden_term = jnp.einsum(
        "kte,kde->td", grad_pre, proj_weight, preferred_element_type=F32
    ).astype(BF16)
    comp_second = rows_of(second)
    hidden_term, comp_second = lax.optimization_barrier((hidden_term, comp_second))
    hidden_part = lax.psum_scatter(hidden_term, "vocab", scatter_dimension=1, tiled=True).astype(F32)
    pres = [grad_pre] + [swap(grad_pre, "dp", dp, s) for s in range(1, dp)]
    pre_all = jnp.concatenate(pres, axis=1)
    hid_all = jnp.concatenate(hid_blocks, axis=0)
    grad_proj = jnp.einsum("td,kte->kde", hid_all, pre_all, preferred_element_type=F32).astype(BF16)

    grad_out = grad_out + contribution(second, comp_second)
    grad_out = (grad_out + back(scaled(comp_rows, coef.reshape(rows)), p_own)).astype(BF16)

    gml_all = jnp.concatenate([c[1] for c in scals], axis=1)
    grad_mix = lax.dot_general(
        hid_all.astype(F32), gml_all, (((0,), (1,)), ((), ())), precision=lax.Precision.HIGHEST
    )
    mix_rows = lax.dynamic_slice_in_dim(mix_weight, vi * cols, cols, 0).astype(F32)
    mix_term = lax.dot_general(
        gml, mix_rows, (((0,), (1,)), ((), ())), precision=lax.Precision.HIGHEST
    )
    grad_hidden = (hidden_part + mix_term).astype(BF16)
    return grad_hidden, grad_mix, grad_proj, grad_out


def solution(mesh):
    dp, nv = mesh.shape["dp"], mesh.shape["vocab"]

    def body(*args):
        return shards(dp, nv, *args)

    return jax.shard_map(
        body,
        mesh=mesh,
        in_specs=(
            P("dp", None),
            P(),
            P(None, None, "vocab"),
            P(None, "vocab"),
            P("dp", None),
            P("dp"),
            P("dp"),
        ),
        out_specs=(P("dp", "vocab"), P("dp", None), P(None, "dp", "vocab"), P("dp", "vocab")),
        check_vma=False,
    )
```
